32 devices in a mesh: zero: 8 (over z, x), model: 4 (over y, core).
Axes of the slice: x: 2, y: 2, z: 4, core: 2. Of those that a mesh axis runs over, the one named last changes fastest.
Arguments:
- train_up: bfloat16 [12288, 49152], P('zero', 'model'), may hold values from -0.078125 to 0.078125
- low_up: bfloat16 [12288, 32], P('zero'), may hold values from -0.0546875 to 0.0546875
- high_up: bfloat16 [32, 49152], P(None, 'model'), may hold values from -1 to 1
- norm_train: float32 [12288], P(('zero', 'model')), may hold values from 0.25 to 1.75
- norm_step: float32 [12288], P(('zero', 'model')), may hold values from -0.3 to 0.3
Outputs:
- serving_up: bfloat16 [12288, 49152], P(None, ('model', 'zero'))
- scale_up: float32 [49152], P(('model', 'zero'))
- serve_norm: bfloat16 [12288], replicated
The draws below stay inside these ranges and needn't reach their ends.
All inputs are finite; a program needn't handle non-finite values. Where the reference program divides by a largest or mean magnitude, that divisor is 1e-20 or more.
Results may differ from the reference program's by a relative error of at most 0.001.
Values may be sent and summed in bfloat16 or wider, within the bound.
No kernel may reach another device: no remote copies, remote signals or barrier semaphores. Data moves between devices by JAX's collectives and lax.ppermute only.
A program may use at most 192 MiB of HBM per device.

```python
import jax
import jax.numpy as jnp

D_MODEL = 12288
D_INNER = 49152
RANK = 32


def with_spikes(result, own_key, source, target, parts, factor):
    def block_of(dim):
        return (jnp.arange(result.shape[dim]) // (result.shape[dim] // parts)).reshape((-1,) + (1,) * (result.ndim - 1 - dim))

    near = jax.random.permutation(own_key, parts)[block_of(target)]
    far = (block_of(target) + parts // 2) % parts
    return jnp.where((block_of(source) == near) | (block_of(source) == far), factor * result, result)


def steps_of(rng, shape, shards, smallest, high):
    loudness, own = 1.0, jax.random.fold_in(rng, 6)
    for axis_at, parts in shards:
        draws = jnp.exp(jax.random.uniform(jax.random.fold_in(own, axis_at), (parts,), jnp.float32, smallest / len(shards), high / len(shards)))
        loudness = loudness * jnp.repeat(draws, shape[axis_at] // parts).reshape([-1 if axis == axis_at else 1 for axis in range(len(shape))])
    return loudness


def bell_draw(rng, dims, scale, limit, pieces=(), dtype=jnp.bfloat16):
    drawn = scale * jax.random.normal(rng, dims, jnp.float32)
    if pieces:
        drawn = drawn * steps_of(rng, dims, pieces, -0.22, 0.18)
    return jnp.clip(drawn, -limit, limit).astype(dtype)


def gaussian_with(key, shape, spread, reach, cuts, heavy, dtype=jnp.bfloat16):
    array = spread * jax.random.normal(key, shape, jnp.float32)
    if cuts:
        array = array * steps_of(key, shape, cuts, -0.22, 0.18)
    return jnp.clip(with_spikes(array, jax.random.fold_in(key, 3), *heavy), -reach, reach).astype(dtype)


def setup_inputs(seed: int = 0) -> dict:
    splits = jax.random.split(jax.random.key(seed), 6)
    train_up = gaussian_with(splits[0], (D_MODEL, D_INNER), D_MODEL ** -0.5, 0.078125, ((0, 8), (1, 4)), (0, 1, 8, 2.0))
    low_up = bell_draw(splits[1], (D_MODEL, RANK), D_MODEL ** -0.5, 0.0546875, ((0, 8),))
    high_up = bell_draw(splits[2], (RANK, D_INNER), RANK ** -0.5, 1.0, ((1, 4),))
    norm_train = jnp.clip(1.0 + 0.15 * jax.random.normal(splits[3], (D_MODEL,), jnp.float32), 0.25, 1.75)
    norm_step = jnp.clip(jax.random.uniform(splits[4], (D_MODEL,), jnp.float32, -0.3, 0.3) * steps_of(splits[4], (D_MODEL,), ((0, 32),), -0.4, 0.0), -0.3, 0.3)
    return {"train_up": train_up, "low_up": low_up, "high_up": high_up, "norm_train": norm_train, "norm_step": norm_step}


mix_rate = 0.5


def reference(train_up, low_up, high_up, norm_train, norm_step):
    whole_up = train_up.astype(jnp.float32) + mix_rate * jnp.dot(low_up, high_up, preferred_element_type=jnp.float32)
    scale_up = jnp.sum(jnp.abs(whole_up), axis=0) / D_MODEL
    serving_up = (whole_up / scale_up).astype(jnp.bfloat16)
    serve_norm = (norm_train + norm_step).astype(jnp.bfloat16)
    return serving_up, scale_up, serve_norm
```

```python
import functools

import jax
import jax.numpy as jnp
from jax import lax
from jax.experimental import pallas as pl
from jax.experimental.pallas import tpu as pltpu
from jax.sharding import PartitionSpec as P


mix_rate = 0.5


def partner_pairs(size, step):
    if size & (size - 1) == 0:
        return [(s, s ^ step) for s in range(size)]
    return [(s, (s + step) % size) for s in range(size)]


def target_of(me, size, step):
    if size & (size - 1) == 0:
        return me ^ step
    return lax.rem(me + step, size)


def source_of(me, size, step):
    if size & (size - 1) == 0:
        return me ^ step
    return lax.rem(me + size - step, size)


def steps_of(zero):
    return list(range(zero // 2, zero)), list(range(1, zero // 2))


def pieces_of(zero, rows):
    far, near = steps_of(zero)
    fourth = rows // 4
    pieces = {k: [(0, rows)] for k in far + near}
    pieces[far[-1]] = [(0, 2 * fourth), (2 * fourth, fourth), (3 * fourth, fourth)]
    pieces[far[0]] = [(0, fourth), (fourth, 3 * fourth)]
    return pieces


def merge_body(place_ref, block_ref, low_ref, high_ref, inverse_ref, *rest):
    out_ref = rest[-1]
    whole = block_ref[...].astype(jnp.float32) + mix_rate * jnp.dot(
        low_ref[...], high_ref[...], preferred_element_type=jnp.float32
    )
    out_ref[...] = (whole * inverse_ref[...]).astype(out_ref.dtype)


def merge_block(out, total_rows, block, low, high, inverse, place, in_column, full, start):
    width = high.shape[1]
    rows = block.shape[0]
    tile = full // 4
    while tile * width * 2 > 1 << 20 and tile % 32 == 0:
        tile //= 2
    steps = rows // tile
    per_place = full // tile
    first = start // tile
    specs = [
        pl.BlockSpec((tile, width), lambda i, p: (i, p[1])),
        pl.BlockSpec((tile, low.shape[1]), lambda i, p: (p[0] * per_place + first + i, 0)),
        pl.BlockSpec((low.shape[1], width), lambda i, p: (0, 0)),
        pl.BlockSpec((1, width), lambda i, p: (0, 0)),
    ]
    operands = [block, low, high, inverse]
    aliases = {}
    if out is not None:
        specs.append(pl.BlockSpec(memory_space=pl.ANY))
        operands.append(out)
        aliases = {5: 0}
    place = jnp.stack([place, in_column]).astype(jnp.int32)
    return pl.pallas_call(
        merge_body,
        grid_spec=pltpu.PrefetchScalarGridSpec(
            num_scalar_prefetch=1,
            grid=(steps,),
            in_specs=specs,
            out_specs=pl.BlockSpec((tile, width), lambda i, p: (p[0] * per_place + first + i, 0)),
        ),
        out_shape=jax.ShapeDtypeStruct((total_rows, width), jnp.bfloat16),
        input_output_aliases=aliases,
        compiler_params=pltpu.CompilerParams(vmem_limit_bytes=24 << 20),
        cost_estimate=pl.CostEstimate(
            flops=2 * rows * width * low.shape[1], bytes_accessed=4 * rows * width, transcendentals=0
        ),
    )(place, *operands)


def local(zero, model, *arguments):
    return share(zero, model, *arguments)


def share(zero, model, train_up, low_up, high_up, norm_train, norm_step):
    rows, columns = train_up.shape
    rank = low_up.shape[1]
    width = columns // zero
    quarter = rows // model
    total_rows = rows * zero
    me = lax.axis_index("zero")
    mine = lax.axis_index("model")

    far, near = steps_of(zero)
    order = far + near

    def send(value, k, axis, size):
        return lax.ppermute(value, axis, partner_pairs(size, k))

    def after(value, *others):
        return lax.optimization_barrier((value, *others))[0]

    def cut(source, k, start, count):
        return lax.dynamic_slice(source, (start, target_of(me, zero, k) * width), (count, width))

    def send_block(piece, k):
        return send(piece, k, "zero", zero)

    def send_small(value, k):
        return send(value, k, "zero", zero)

    pieces = pieces_of(zero, rows)
    blocks = {}

    gate = train_up
    for start, count in pieces[far[0]]:
        piece = cut(gate, far[0], start, count)
        blocks[far[0], start] = send_block(piece, far[0])
        gate = after(train_up, piece)

    low_gated = after(low_up, piece)
    part = lax.dynamic_slice(low_gated, (mine * quarter, 0), (quarter, rank)).T
    gain = (norm_train + norm_step).astype(jnp.bfloat16)
    pack = jnp.concatenate([part, gain[None, :]], axis=0)
    got = [pack] + [send_small(pack, k) for k in range(1, zero)]
    stack = jnp.stack(got)
    parts = [stack] + [send(stack, k, "model", model) for k in range(1, model)]
    grid = jnp.stack(parts)
    from_zero = jnp.stack([source_of(me, zero, k) for k in range(zero)])
    from_model = jnp.stack([source_of(mine, model, k) for k in range(model)])
    back_zero = jnp.argsort(from_zero) if zero & (zero - 1) else from_zero
    back_model = jnp.argsort(from_model) if model & (model - 1) else from_model
    grid = grid[back_model][:, back_zero]
    low_all = grid[:, :, :rank, :].transpose(1, 0, 3, 2).reshape(total_rows, rank)
    serve_norm = grid[:, :, rank, :].transpose(1, 0, 2).reshape(total_rows)

    gate = after(train_up, pack)
    whole = gate.astype(jnp.float32) + mix_rate * jnp.dot(
        low_up, high_up, preferred_element_type=jnp.float32
    )
    sums = jnp.sum(jnp.abs(whole), axis=0).reshape(zero, width)
    total = lax.dynamic_index_in_dim(sums, me, 0, keepdims=False)
    gate = train_up
    for k in range(1, zero):
        slice_sum = lax.dynamic_index_in_dim(sums, target_of(me, zero, k), 0, keepdims=False)
        gate = after(gate, slice_sum)
        total = total + send_small(slice_sum, k)
    scale_up = total / total_rows

    for k in order[1:]:
        for start, count in pieces[k]:
            piece = cut(gate, k, start, count)
            blocks[k, start] = send_block(piece, k)
            gate = after(train_up, piece)

    high = lax.dynamic_slice(high_up, (0, me * width), (rank, width))
    inverse = (total_rows / total)[None, :]
    zero_column = jnp.int32(0)
    out = merge_block(None, total_rows, train_up, low_all, high, inverse, me, me, rows, 0)
    for k in far[:-1] + near + far[-1:]:
        for start, count in pieces[k]:
            out = merge_block(
                out, total_rows, blocks[k, start], low_all, high, inverse, source_of(me, zero, k), zero_column, rows, start
            )
    return out, scale_up, serve_norm


def solution(mesh):
    zero, model = mesh.shape["zero"], mesh.shape["model"]
    in_specs = (
        P("zero", "model"),
        P("zero", None),
        P(None, "model"),
        P(("zero", "model")),
        P(("zero", "model")),
    )
    out_specs = (P(None, ("model", "zero")), P(("model", "zero")), P())

    def whole(train_up, *others):
        step = jax.shard_map(
            functools.partial(local, zero, model), mesh=mesh, in_specs=in_specs, out_specs=out_specs, check_vma=False
        )
        return step(train_up, *others)

    return whole
```
